32 devices in a mesh: expert: 4 (over y, core), shard: 8 (over z, x).
Axes of the slice: x: 2, y: 2, z: 4, core: 2. Of those that a mesh axis runs over, the one named last changes fastest.
Arguments:
- params: float32 [3, 4, 6144, 256], P(None, 'expert', 'shard'), may hold values from -3 to 3
- grads: float32 [3, 4, 6144, 256], P(None, 'expert', 'shard')
- moment: float32 [3, 4, 6144, 256], P(None, 'expert', 'shard'), may hold values from -0.6 to 0.6
- second: float32 [3, 4, 64], P(None, 'expert'), may hold values from 0.002 to 0.2
- step: int32 [1], replicated, may hold values from 1 to 8
- block_map: int32 [256], replicated, may hold values from 0 to 63, never falling along the last dimension, each value on 1 to 8 neighbouring positions
Outputs:
- new_weights: bfloat16 [3, 4, 6144, 256], P(None, 'expert')
- new_moment: float32 [3, 4, 6144, 256], P(None, 'expert', 'shard')
- new_second: float32 [3, 4, 64], P(None, 'expert')
The draws below stay inside these ranges and needn't reach their ends.
Inputs may be any that keep to these rules, and one draw needn't show every extreme that they name: `block_map`: every block holds at least one neuron and at most 8.
All inputs are finite; a program needn't handle non-finite values.
Results may differ from the reference program's by a relative error of at most 0.001.
Values may be sent and summed in bfloat16 or wider, within the bound.
A program may use at most 64 MiB of HBM per device.

```python
import math
import jax
import jax.numpy as jnp
import numpy as np
from jax import lax

D = 6144
NEUR = 256
NBLK = 64
EXPERTS = 4


def draw_grads(key, part):
    keys = jax.random.split(key, 4)
    row_place = jnp.arange(D, dtype=jnp.float32) / D
    expert_place = jnp.arange(EXPERTS, dtype=jnp.float32) / EXPERTS
    noise = jax.random.normal(keys[0], (3, EXPERTS, D, NEUR), jnp.float32)
    row_scale = jnp.power(10.0, 0.5 * row_place + 0.5 * jax.random.uniform(keys[1], (D,), jnp.float32))
    column_scale = jnp.power(10.0, jax.random.uniform(keys[2], (NEUR,), jnp.float32))
    expert_scale = jnp.power(10.0, 0.25 * expert_place + 0.25 * jax.random.uniform(keys[3], (EXPERTS,), jnp.float32))
    return noise * row_scale[None, None, :, None] * column_scale[None, None, None, :] * expert_scale[None, :, None, None]


def block_scale(stream_key, dims, cuts, low, top_value):
    level, own = 1.0, jax.random.fold_in(stream_key, 6)
    for position, blocks in cuts:
        heights = jnp.exp(jax.random.uniform(jax.random.fold_in(own, position), (blocks,), jnp.float32, low / len(cuts), top_value / len(cuts)))
        level = level * jnp.repeat(heights, dims[position] // blocks).reshape([-1 if axis == position else 1 for axis in range(len(dims))])
    return level


def length_profile(count, total, reach, skew):
    loads = [(1 << 20) // math.isqrt(rank ** skew) + 1 for rank in range(2, count + 1)]
    rest, holding = total - reach - (count - 1), [1] * (count - 1)
    while rest > 0:
        candidates = [i for i in range(count - 1) if holding[i] < reach]
        pool, remaining = sum([loads[i] for i in candidates]), rest
        for i in candidates:
            addition = min(reach - holding[i], max(1, remaining * loads[i] // pool), rest)
            holding[i] = holding[i] + addition
            rest = rest - addition
    return np.array([reach] + holding)


def uneven(key, amount, total, reach, skew):
    if amount == 2:
        one = jax.random.randint(key, (), max(1, total - reach), min(reach, total - 1) + 1)
        return jnp.stack([one, total - one])
    sizes = jnp.asarray(length_profile(amount, total, reach, skew), jnp.int32)
    couples = (amount - 1) // 2
    donor, receiver = sizes[1:1 + 2 * couples:2], sizes[2:2 + 2 * couples:2]
    margin = jnp.minimum(donor - 1, reach - receiver)
    moved = jax.random.randint(jax.random.fold_in(key, 1), (couples,), 0, 1 << 20) % (margin + 1)
    sizes = sizes.at[1:1 + 2 * couples:2].set(donor - moved).at[2:2 + 2 * couples:2].set(receiver + moved)
    return sizes[jax.random.permutation(jax.random.fold_in(key, 2), amount)]


def centred(rng, shape, width, reach, pieces=(), kind=jnp.bfloat16):
    level = block_scale(rng, shape, pieces, -0.22, 0.18) if pieces else 1.0
    drawn = jax.random.normal(rng, shape, jnp.float32) * width * level
    return jnp.minimum(jnp.maximum(drawn, -reach), reach).astype(kind)


def setup_inputs(seed: int = 0) -> dict:
    key_list = jax.random.split(jax.random.key(seed), 7)
    return {
        "params": centred(key_list[0], (3, EXPERTS, D, NEUR), 0.5, 3.0, ((1, 4), (2, 8)), jnp.float32),
        "grads": draw_grads(jax.random.fold_in(key_list[6], 71), 0),
        "moment": centred(key_list[2], (3, EXPERTS, D, NEUR), 0.1, 0.6, ((1, 4), (2, 8)), jnp.float32),
        "second": jnp.clip(jnp.exp(math.log(0.2) - 4.6051702 * jax.random.uniform(key_list[3], (3, EXPERTS, NBLK), jnp.float32) ** block_scale(key_list[3], (3, EXPERTS, NBLK), ((1, 4),), -0.2, 0.2)), 0.002, 0.2),
        "step": jax.random.randint(key_list[4], (1,), 1, 9).astype(jnp.int32),
        "block_map": jnp.searchsorted(jnp.cumsum(uneven(key_list[5], NBLK, NEUR, 8, 1)), jnp.arange(NEUR), side="right").astype(jnp.int32),
    }


LEARN_RATE = 0.05
DECAY_WEIGHT = 0.1
BETA_FIRST = 0.9
BETA_SECOND = 0.95
epsilon = 1e-08

def reference(params, grads, moment, second, step, block_map):
    member_table = (block_map[:, None] == jnp.arange(NBLK, dtype=jnp.int32)[None, :]).astype(jnp.float32)
    members = lax.optimization_barrier(jnp.sum(member_table, axis=0))
    squares = lax.optimization_barrier(jnp.sum(grads * grads, axis=2))
    block_sums = jnp.einsum('ken,nb->keb', squares, member_table, precision=lax.Precision.HIGHEST)
    total = jnp.sum(block_sums)
    limit = math.sqrt(3 * EXPERTS * D * NEUR)
    clip = jnp.minimum(1.0, limit / (jnp.sqrt(total) + 1e-06))
    new_second = BETA_SECOND * second + (1.0 - BETA_SECOND) * clip * clip * block_sums / (D * members)
    new_moment = BETA_FIRST * moment + (1.0 - BETA_FIRST) * clip * grads
    step_value = step[0].astype(jnp.float32)
    first_fix = 1.0 - jnp.power(jnp.float32(BETA_FIRST), step_value)
    second_fix = 1.0 - jnp.power(jnp.float32(BETA_SECOND), step_value)
    divisor = jnp.sqrt(new_second / second_fix) + epsilon
    by_neuron = jnp.einsum('keb,nb->ken', divisor, member_table, precision=lax.Precision.HIGHEST)
    updated = params * (1.0 - LEARN_RATE * DECAY_WEIGHT) - LEARN_RATE * (new_moment / first_fix) / by_neuron[:, :, None, :]
    return (updated.astype(jnp.bfloat16), new_moment, new_second)
```

```python
import functools
import math

import jax
import jax.numpy as jnp
from jax import lax
from jax.experimental import pallas as pl
from jax.experimental.pallas import tpu as pltpu
from jax.sharding import PartitionSpec as P

LEARN_RATE = 0.05
DECAY_WEIGHT = 0.1
BETA_FIRST = 0.9
BETA_SECOND = 0.95
epsilon = 1e-08
MESH = pl.DeviceIdType.MESH
LANES = 128
STRIP = 64


def ring_position(shard, n):
    if n % 2:
        return shard
    row, side = shard // 2, shard % 2
    return jnp.where(side == 0, row, n - 1 - row)


def ring_shard(position, n):
    position = lax.rem(position + 2 * n, n)
    if n % 2:
        return position
    return jnp.where(position < n // 2, 2 * position, 2 * (n - 1 - position) + 1)


def kernel(
    experts,
    shards,
    limit,
    params,
    grads,
    moment,
    second,
    step,
    block_map,
    weights,
    new_moment,
    new_second,
    p_buf,
    g_buf,
    m_buf,
    tile,
    total_row,
    tiles,
    totals,
    load_sem,
    tile_send,
    tile_recv,
    total_send,
    total_recv,
    ring_send,
    ring_recv,
):
    e = lax.axis_index("expert")
    s = lax.axis_index("shard")
    devices = experts * shards
    me = e * shards + s
    mats, rows, neurons = p_buf.shape
    width = rows * shards
    folds = neurons // LANES

    for k in range(mats):
        pltpu.make_async_copy(grads.at[k], g_buf.at[k], load_sem.at[0, k]).start()
    for k in range(mats):
        pltpu.make_async_copy(moment.at[k], m_buf.at[k], load_sem.at[1, k]).start()
        pltpu.make_async_copy(params.at[k], p_buf.at[k], load_sem.at[2, k]).start()

    barrier = pltpu.get_barrier_semaphore()

    def greet(j, carry):
        other = lax.rem(me + j, devices)
        pl.semaphore_signal(
            barrier,
            inc=1,
            device_id=(other // shards, lax.rem(other, shards)),
            device_id_type=MESH,
        )
        return carry

    lax.fori_loop(1, devices, greet, 0)

    blocks = second.shape[1]
    table = (
        lax.broadcasted_iota(jnp.int32, (blocks, neurons), 0) == block_map[...]
    ).astype(jnp.float32)
    members = lax.dot_general(
        jnp.ones((8, neurons), jnp.float32),
        table,
        (((1,), (1,)), ((), ())),
        precision=lax.Precision.HIGHEST,
    )[:mats]
    step_value = jnp.full((1, LANES), step[0].astype(jnp.float32))
    first_fix = 1.0 - jnp.power(jnp.full((1, LANES), BETA_FIRST, jnp.float32), step_value)
    second_fix = 1.0 - jnp.power(jnp.full((1, LANES), BETA_SECOND, jnp.float32), step_value)
    first_fix = first_fix[:, :1]
    second_fix = second_fix[:, :1]

    squares = []
    for k in range(mats):
        pltpu.make_async_copy(grads.at[k], g_buf.at[k], load_sem.at[0, k]).wait()

        def add_squares(i, acc, k=k):
            g = g_buf[k, pl.ds(pl.multiple_of(i * STRIP, STRIP), STRIP), :]
            return acc + jnp.sum((g * g).reshape(STRIP // 8, 8, neurons), axis=0)

        acc = lax.fori_loop(0, rows // STRIP, add_squares, jnp.zeros((8, neurons), jnp.float32))
        squares.append(jnp.sum(acc, axis=0, keepdims=True))
    parts = [sq[:, f * LANES : (f + 1) * LANES] for f in range(folds) for sq in squares]
    own_total = functools.reduce(lambda a, b: a + b, parts)
    own_total = jnp.broadcast_to(jnp.sum(own_total, axis=1, keepdims=True), (1, LANES))
    pad = tile.shape[0] - len(parts)
    if pad:
        parts.append(jnp.zeros((pad, LANES), jnp.float32))
    own_tile = jnp.concatenate(parts, axis=0)
    tile[...] = own_tile
    total_row[...] = own_total
    tiles[s] = own_tile
    totals[me] = own_total

    pl.semaphore_wait(barrier, devices - 1)

    def tile_copy(j, arriving):
        to = lax.rem(s + j, shards)
        origin = lax.rem(s + shards - j, shards) if arriving else s
        return pltpu.make_async_remote_copy(
            src_ref=tile,
            dst_ref=tiles.at[origin],
            send_sem=tile_send.at[j],
            recv_sem=tile_recv.at[j],
            device_id=(e, to),
            device_id_type=MESH,
        )

    def total_copy(j, arriving):
        other = lax.rem(me + j, devices)
        origin = lax.rem(me + devices - j, devices) if arriving else me
        return pltpu.make_async_remote_copy(
            src_ref=total_row,
            dst_ref=totals.at[origin],
            send_sem=total_send.at[j],
            recv_sem=total_recv.at[j],
            device_id=(other // shards, lax.rem(other, shards)),
            device_id_type=MESH,
        )

    def start_total(j, carry):
        total_copy(j, False).start()
        return carry

    def start_tile(j, carry):
        tile_copy(j, False).start()
        return carry

    def wait_total(j, carry):
        total_copy(j, True).wait_recv()
        return carry

    def wait_tile(j, carry):
        tile_copy(j, True).wait_recv()
        return carry

    def sent_total(j, carry):
        total_copy(j, False).wait_send()
        return carry

    def sent_tile(j, carry):
        tile_copy(j, False).wait_send()
        return carry

    lax.fori_loop(1, devices, start_total, 0)
    lax.fori_loop(1, shards, start_tile, 0)
    lax.fori_loop(1, devices, wait_total, 0)
    lax.fori_loop(1, shards, wait_tile, 0)

    total = jnp.sum(totals[...], axis=0)
    clip = jnp.minimum(1.0, limit / (jnp.sqrt(total) + 1e-06))[:, :1]
    all_tile = jnp.sum(tiles[...], axis=0)
    square = jnp.concatenate(
        [all_tile[f * mats : (f + 1) * mats] for f in range(folds)], axis=1
    )
    block_sums = lax.dot_general(
        square, table, (((1,), (1,)), ((), ())), precision=lax.Precision.HIGHEST
    )
    updated = BETA_SECOND * second[...] + (1.0 - BETA_SECOND) * clip * clip * block_sums / (
        width * members
    )
    new_second[...] = updated
    divisor = jnp.sqrt(updated / second_fix) + epsilon
    by_neuron = lax.dot_general(
        divisor, table, (((1,), (0,)), ((), ())), precision=lax.Precision.HIGHEST
    )
    rate = LEARN_RATE / (first_fix * by_neuron)
    grad_scale = (1.0 - BETA_FIRST) * clip

    place = ring_position(s, shards)
    half = rows // 2
    right = ring_shard(place + 1, shards)
    left = ring_shard(place - 1, shards)
    far, near = shards // 2, (shards - 1) // 2
    hops = ((far, near), (near, far))

    def ring_copy(way, hop, k, part, arriving):
        back = hop + (1 if arriving else 0)
        origin = ring_shard(place - back if way == 0 else place + back, shards)
        block = weights.at[k, pl.ds(pl.multiple_of(origin * rows + part * half, half), half), :]
        return pltpu.make_async_remote_copy(
            src_ref=block,
            dst_ref=block,
            send_sem=ring_send.at[way, hop, 2 * k + part],
            recv_sem=ring_recv.at[way, hop, 2 * k + part],
            device_id=(e, right if way == 0 else left),
            device_id_type=MESH,
        )

    for k in range(mats):
        pltpu.make_async_copy(moment.at[k], m_buf.at[k], load_sem.at[1, k]).wait()
        pltpu.make_async_copy(params.at[k], p_buf.at[k], load_sem.at[2, k]).wait()
        rate_k = rate[k : k + 1]
        for part in range(2):

            def update(i, carry, k=k, part=part, rate_k=rate_k):
                at = pl.multiple_of(part * half + i * STRIP, STRIP)
                strip = pl.ds(at, STRIP)
                value = BETA_FIRST * m_buf[k, strip, :] + grad_scale * g_buf[k, strip, :]
                new_moment[k, strip, :] = value
                out = p_buf[k, strip, :] * (1.0 - LEARN_RATE * DECAY_WEIGHT) - rate_k * value
                weights[k, pl.ds(pl.multiple_of(s * rows + at, STRIP), STRIP), :] = out.astype(
                    jnp.bfloat16
                )
                return carry

            lax.fori_loop(0, half // STRIP, update, 0)
            for way in range(2):
                if hops[way][part] > 0:
                    ring_copy(way, 0, k, part, False).start()

    lax.fori_loop(1, devices, sent_total, 0)
    lax.fori_loop(1, shards, sent_tile, 0)

    for hop in range(far):
        for k in range(mats):
            for part in range(2):
                for way in range(2):
                    if hop < hops[way][part]:
                        ring_copy(way, hop, k, part, True).wait_recv()
                        if hop + 1 < hops[way][part]:
                            ring_copy(way, hop + 1, k, part, False).start()
    for hop in range(far):
        for k in range(mats):
            for part in range(2):
                for way in range(2):
                    if hop < hops[way][part]:
                        ring_copy(way, hop, k, part, False).wait_send()


def store_kernel(weights, moment, second, weights_out, moment_out, second_out, sem):
    mats = weights.shape[0]
    copies = [
        pltpu.make_async_copy(weights.at[k], weights_out.at[k], sem.at[0, k]) for k in range(mats)
    ] + [pltpu.make_async_copy(moment.at[k], moment_out.at[k], sem.at[1, k]) for k in range(mats)]
    for copy in copies:
        copy.start()
    second_out[...] = second[...]
    for copy in copies:
        copy.wait()


def body(params, grads, moment, second, step, block_map):
    experts, shards = lax.axis_size("expert"), lax.axis_size("shard")
    mats, own, rows, neurons = params.shape
    blocks = second.shape[2]
    width = rows * shards
    devices = experts * shards
    limit = math.sqrt(mats * experts * own * width * neurons)
    flat = (mats, own * rows, neurons)
    far = max(shards // 2, 1)
    tile_rows = -(-mats * (neurons // LANES) // 8) * 8
    hbm = pl.BlockSpec(memory_space=pltpu.HBM)
    vmem = pl.BlockSpec(memory_space=pltpu.VMEM)
    smem = pl.BlockSpec(memory_space=pltpu.SMEM)
    dma = pltpu.SemaphoreType.DMA
    shapes = (
        jax.ShapeDtypeStruct((mats, width, neurons), jnp.bfloat16),
        jax.ShapeDtypeStruct(flat, jnp.float32),
        jax.ShapeDtypeStruct((mats, blocks), jnp.float32),
    )
    results = pl.pallas_call(
        functools.partial(kernel, experts, shards, limit),
        out_shape=shapes,
        in_specs=[hbm, hbm, hbm, vmem, smem, vmem],
        out_specs=(vmem, vmem, vmem),
        scratch_shapes=[
            pltpu.VMEM(flat, jnp.float32),
            pltpu.VMEM(flat, jnp.float32),
            pltpu.VMEM(flat, jnp.float32),
            pltpu.VMEM((tile_rows, LANES), jnp.float32),
            pltpu.VMEM((1, LANES), jnp.float32),
            pltpu.VMEM((shards, tile_rows, LANES), jnp.float32),
            pltpu.VMEM((devices, 1, LANES), jnp.float32),
            dma((3, mats)),
            dma((shards,)),
            dma((shards,)),
            dma((devices,)),
            dma((devices,)),
            dma((2, far, 2 * mats)),
            dma((2, far, 2 * mats)),
        ],
        compiler_params=pltpu.CompilerParams(
            collective_id=0, has_side_effects=True, vmem_limit_bytes=32 * 1024 * 1024
        ),
    )(
        params.reshape(flat),
        grads.reshape(flat),
        moment.reshape(flat),
        second.reshape(mats, blocks),
        step,
        block_map.reshape(1, neurons),
    )
    weights, new_moment, new_second = pl.pallas_call(
        store_kernel,
        out_shape=shapes,
        in_specs=[vmem, vmem, vmem],
        out_specs=(hbm, hbm, vmem),
        scratch_shapes=[dma((2, mats))],
        compiler_params=pltpu.CompilerParams(vmem_limit_bytes=8 * 1024 * 1024),
    )(*results)
    return (
        weights.reshape(mats, own, width, neurons),
        new_moment.reshape(mats, own, rows, neurons),
        new_second.reshape(mats, own, blocks),
    )


def solution(mesh):
    placed = (
        P(None, "expert", "shard", None),
        P(None, "expert", "shard", None),
        P(None, "expert", "shard", None),
        P(None, "expert", None),
        P(),
        P(),
    )
    return jax.shard_map(
        body,
        mesh=mesh,
        in_specs=placed,
        out_specs=(
            P(None, "expert", None, None),
            P(None, "expert", "shard", None),
            P(None, "expert", None),
        ),
        check_vma=False,
    )
```

```python
import functools
import math

import jax
import jax.numpy as jnp
from jax import lax
from jax.experimental import pallas as pl
from jax.experimental.pallas import tpu as pltpu
from jax.sharding import PartitionSpec as P

LEARN_RATE = 0.05
DECAY_WEIGHT = 0.1
BETA_FIRST = 0.9
BETA_SECOND = 0.95
epsilon = 1e-08
MESH = pl.DeviceIdType.MESH
LANES = 128
STRIP = 64


def ring_position(shard, n):
    if n % 2:
        return shard
    row, side = shard // 2, shard % 2
    return jnp.where(side == 0, row, n - 1 - row)


def ring_shard(position, n):
    position = lax.rem(position + 2 * n, n)
    if n % 2:
        return position
    return jnp.where(position < n // 2, 2 * position, 2 * (n - 1 - position) + 1)


def kernel(
    experts,
    shards,
    limit,
    params,
    grads,
    moment,
    second,
    step,
    block_map,
    weights,
    new_moment,
    new_second,
    p_buf,
    g_buf,
    m_buf,
    s_buf,
    map_buf,
    tile,
    total_row,
    tiles,
    totals,
    load_sem,
    small_sem,
    tile_send,
    tile_recv,
    total_send,
    total_recv,
    ring_send,
    ring_recv,
):
    e = lax.axis_index("expert")
    s = lax.axis_index("shard")
    devices = experts * shards
    me = e * shards + s
    mats, rows, neurons = p_buf.shape
    width = rows * shards
    folds = neurons // LANES

    for k in range(mats):
        pltpu.make_async_copy(grads.at[k], g_buf.at[k], load_sem.at[0, k]).start()
    for k in range(mats):
        pltpu.make_async_copy(moment.at[k], m_buf.at[k], load_sem.at[1, k]).start()
        pltpu.make_async_copy(params.at[k], p_buf.at[k], load_sem.at[2, k]).start()

    map_load = pltpu.make_async_copy(block_map, map_buf, small_sem.at[0])
    second_load = pltpu.make_async_copy(second, s_buf, small_sem.at[1])
    map_load.start()
    second_load.start()

    barrier = pltpu.get_barrier_semaphore()

    def greet(j, carry):
        other = lax.rem(me + j, devices)
        pl.semaphore_signal(
            barrier,
            inc=1,
            device_id=(other // shards, lax.rem(other, shards)),
            device_id_type=MESH,
        )
        return carry

    lax.fori_loop(1, devices, greet, 0)

    blocks = second.shape[2]
    map_load.wait()
    second_load.wait()
    table = (
        lax.broadcasted_iota(jnp.int32, (blocks, neurons), 0) == map_buf[...]
    ).astype(jnp.float32)
    members = lax.dot_general(
        jnp.ones((8, neurons), jnp.float32),
        table,
        (((1,), (1,)), ((), ())),
        precision=lax.Precision.HIGHEST,
    )[:mats]
    step_value = jnp.full((1, LANES), step[0].astype(jnp.float32))
    first_fix = 1.0 - jnp.power(jnp.full((1, LANES), BETA_FIRST, jnp.float32), step_value)
    second_fix = 1.0 - jnp.power(jnp.full((1, LANES), BETA_SECOND, jnp.float32), step_value)
    first_fix = first_fix[:, :1]
    second_fix = second_fix[:, :1]

    squares = []
    for k in range(mats):
        pltpu.make_async_copy(grads.at[k], g_buf.at[k], load_sem.at[0, k]).wait()

        def add_squares(i, acc, k=k):
            g = g_buf[k, pl.ds(pl.multiple_of(i * STRIP, STRIP), STRIP), :]
            return acc + jnp.sum((g * g).reshape(STRIP // 8, 8, neurons), axis=0)

        acc = lax.fori_loop(0, rows // STRIP, add_squares, jnp.zeros((8, neurons), jnp.float32))
        squares.append(jnp.sum(acc, axis=0, keepdims=True))
    parts = [sq[:, f * LANES : (f + 1) * LANES] for f in range(folds) for sq in squares]
    own_total = functools.reduce(lambda a, b: a + b, parts)
    own_total = jnp.broadcast_to(jnp.sum(own_total, axis=1, keepdims=True), (1, LANES))
    pad = tile.shape[0] - len(parts)
    if pad:
        parts.append(jnp.zeros((pad, LANES), jnp.float32))
    own_tile = jnp.concatenate(parts, axis=0)
    tile[...] = own_tile
    total_row[...] = own_total
    tiles[s] = own_tile
    totals[me] = own_total

    pl.semaphore_wait(barrier, devices - 1)

    def tile_copy(j, arriving):
        to = lax.rem(s + j, shards)
        origin = lax.rem(s + shards - j, shards) if arriving else s
        return pltpu.make_async_remote_copy(
            src_ref=tile,
            dst_ref=tiles.at[origin],
            send_sem=tile_send.at[j],
            recv_sem=tile_recv.at[j],
            device_id=(e, to),
            device_id_type=MESH,
        )

    def total_copy(j, arriving):
        other = lax.rem(me + j, devices)
        origin = lax.rem(me + devices - j, devices) if arriving else me
        return pltpu.make_async_remote_copy(
            src_ref=total_row,
            dst_ref=totals.at[origin],
            send_sem=total_send.at[j],
            recv_sem=total_recv.at[j],
            device_id=(other // shards, lax.rem(other, shards)),
            device_id_type=MESH,
        )

    def start_total(j, carry):
        total_copy(j, False).start()
        return carry

    def start_tile(j, carry):
        tile_copy(j, False).start()
        return carry

    def wait_total(j, carry):
        total_copy(j, True).wait_recv()
        return carry

    def wait_tile(j, carry):
        tile_copy(j, True).wait_recv()
        return carry

    def sent_total(j, carry):
        total_copy(j, False).wait_send()
        return carry

    def sent_tile(j, carry):
        tile_copy(j, False).wait_send()
        return carry

    lax.fori_loop(1, devices, start_total, 0)
    lax.fori_loop(1, shards, start_tile, 0)
    lax.fori_loop(1, devices, wait_total, 0)
    lax.fori_loop(1, shards, wait_tile, 0)

    total = jnp.sum(totals[...], axis=0)
    clip = jnp.minimum(1.0, limit / (jnp.sqrt(total) + 1e-06))[:, :1]
    all_tile = jnp.sum(tiles[...], axis=0)
    square = jnp.concatenate(
        [all_tile[f * mats : (f + 1) * mats] for f in range(folds)], axis=1
    )
    block_sums = lax.dot_general(
        square, table, (((1,), (1,)), ((), ())), precision=lax.Precision.HIGHEST
    )
    updated = BETA_SECOND * s_buf[:, 0, :] + (1.0 - BETA_SECOND) * clip * clip * block_sums / (
        width * members
    )
    for k in range(mats):
        new_second[k] = updated[k : k + 1]
    divisor = jnp.sqrt(updated / second_fix) + epsilon
    by_neuron = lax.dot_general(
        divisor, table, (((1,), (0,)), ((), ())), precision=lax.Precision.HIGHEST
    )
    rate = LEARN_RATE / (first_fix * by_neuron)
    grad_scale = (1.0 - BETA_FIRST) * clip

    place = ring_position(s, shards)
    half = rows // 2
    right = ring_shard(place + 1, shards)
    left = ring_shard(place - 1, shards)
    far, near = shards // 2, (shards - 1) // 2
    hops = ((far, near), (near, far))

    def ring_copy(way, hop, k, part, arriving):
        back = hop + (1 if arriving else 0)
        origin = ring_shard(place - back if way == 0 else place + back, shards)
        block = weights.at[k, pl.ds(pl.multiple_of(origin * rows + part * half, half), half), :]
        return pltpu.make_async_remote_copy(
            src_ref=block,
            dst_ref=block,
            send_sem=ring_send.at[way, hop, 2 * k + part],
            recv_sem=ring_recv.at[way, hop, 2 * k + part],
            device_id=(e, right if way == 0 else left),
            device_id_type=MESH,
        )

    for k in range(mats):
        pltpu.make_async_copy(moment.at[k], m_buf.at[k], load_sem.at[1, k]).wait()
        pltpu.make_async_copy(params.at[k], p_buf.at[k], load_sem.at[2, k]).wait()
        rate_k = rate[k : k + 1]
        for part in range(2):

            def update(i, carry, k=k, part=part, rate_k=rate_k):
                at = pl.multiple_of(part * half + i * STRIP, STRIP)
                strip = pl.ds(at, STRIP)
                value = BETA_FIRST * m_buf[k, strip, :] + grad_scale * g_buf[k, strip, :]
                new_moment[k, strip, :] = value
                out = p_buf[k, strip, :] * (1.0 - LEARN_RATE * DECAY_WEIGHT) - rate_k * value
                weights[k, pl.ds(pl.multiple_of(s * rows + at, STRIP), STRIP), :] = out.astype(
                    jnp.bfloat16
                )
                return carry

            lax.fori_loop(0, half // STRIP, update, 0)
            for way in range(2):
                if hops[way][part] > 0:
                    ring_copy(way, 0, k, part, False).start()

    lax.fori_loop(1, devices, sent_total, 0)
    lax.fori_loop(1, shards, sent_tile, 0)

    for hop in range(far):
        for k in range(mats):
            for part in range(2):
                for way in range(2):
                    if hop < hops[way][part]:
                        ring_copy(way, hop, k, part, True).wait_recv()
                        if hop + 1 < hops[way][part]:
                            ring_copy(way, hop + 1, k, part, False).start()
    for hop in range(far):
        for k in range(mats):
            for part in range(2):
                for way in range(2):
                    if hop < hops[way][part]:
                        ring_copy(way, hop, k, part, False).wait_send()


def store_kernel(weights, moment, second, weights_out, moment_out, second_out, sem):
    mats = weights.shape[0]
    copies = [
        pltpu.make_async_copy(weights.at[k], weights_out.at[k], sem.at[0, k]) for k in range(mats)
    ] + [pltpu.make_async_copy(moment.at[k], moment_out.at[k], sem.at[1, k]) for k in range(mats)]
    copies.append(pltpu.make_async_copy(second, second_out, sem.at[0, mats]))
    for copy in copies:
        copy.start()
    for copy in copies:
        copy.wait()


def body(params, grads, moment, second, step, block_map):
    experts, shards = lax.axis_size("expert"), lax.axis_size("shard")
    mats, own, rows, neurons = params.shape
    blocks = second.shape[2]
    width = rows * shards
    devices = experts * shards
    limit = math.sqrt(mats * experts * own * width * neurons)
    flat = (mats, own * rows, neurons)
    far = max(shards // 2, 1)
    tile_rows = -(-mats * (neurons // LANES) // 8) * 8
    hbm = pl.BlockSpec(memory_space=pltpu.HBM)
    vmem = pl.BlockSpec(memory_space=pltpu.VMEM)
    smem = pl.BlockSpec(memory_space=pltpu.SMEM)
    dma = pltpu.SemaphoreType.DMA
    shapes = (
        jax.ShapeDtypeStruct((mats, width, neurons), jnp.bfloat16),
        jax.ShapeDtypeStruct(flat, jnp.float32),
        jax.ShapeDtypeStruct((mats, own, blocks), jnp.float32),
    )
    results = pl.pallas_call(
        functools.partial(kernel, experts, shards, limit),
        out_shape=tuple(pltpu.VMEM(shape.shape, shape.dtype) for shape in shapes),
        in_specs=[hbm, hbm, hbm, hbm, smem, hbm],
        out_specs=(vmem, vmem, vmem),
        scratch_shapes=[
            pltpu.VMEM(flat, jnp.float32),
            pltpu.VMEM(flat, jnp.float32),
            pltpu.VMEM(flat, jnp.float32),
            pltpu.VMEM((mats, own, blocks), jnp.float32),
            pltpu.VMEM((1, neurons), jnp.int32),
            pltpu.VMEM((tile_rows, LANES), jnp.float32),
            pltpu.VMEM((1, LANES), jnp.float32),
            pltpu.VMEM((shards, tile_rows, LANES), jnp.float32),
            pltpu.VMEM((devices, 1, LANES), jnp.float32),
            dma((3, mats)),
            dma((2,)),
            dma((shards,)),
            dma((shards,)),
            dma((devices,)),
            dma((devices,)),
            dma((2, far, 2 * mats)),
            dma((2, far, 2 * mats)),
        ],
        compiler_params=pltpu.CompilerParams(
            collective_id=0, has_side_effects=True, vmem_limit_bytes=46 * 1024 * 1024
        ),
    )(
        params.reshape(flat),
        grads.reshape(flat),
        moment.reshape(flat),
        second,
        step,
        block_map.reshape(1, neurons),
    )
    weights, new_moment, new_second = pl.pallas_call(
        store_kernel,
        out_shape=shapes,
        in_specs=[vmem, vmem, vmem],
        out_specs=(hbm, hbm, hbm),
        scratch_shapes=[dma((2, mats + 1))],
        compiler_params=pltpu.CompilerParams(vmem_limit_bytes=8 * 1024 * 1024),
    )(*results)
    return (
        weights.reshape(mats, own, width, neurons),
        new_moment.reshape(mats, own, rows, neurons),
        new_second,
    )


def solution(mesh):
    placed = (
        P(None, "expert", "shard", None),
        P(None, "expert", "shard", None),
        P(None, "expert", "shard", None),
        P(None, "expert", None),
        P(),
        P(),
    )
    return jax.shard_map(
        body,
        mesh=mesh,
        in_specs=placed,
        out_specs=(
            P(None, "expert", None, None),
            P(None, "expert", "shard", None),
            P(None, "expert", None),
        ),
        check_vma=False,
    )
```

```python
import functools
import math

import jax
import jax.numpy as jnp
from jax import lax
from jax.experimental import pallas as pl
from jax.experimental.pallas import tpu as pltpu
from jax.sharding import PartitionSpec as P

LEARN_RATE = 0.05
DECAY_WEIGHT = 0.1
BETA_FIRST = 0.9
BETA_SECOND = 0.95
epsilon = 1e-08
MESH = pl.DeviceIdType.MESH
LANES = 128
STRIP = 64


def ring_position(shard, n):
    if n % 2:
        return shard
    row, side = shard // 2, shard % 2
    return jnp.where(side == 0, row, n - 1 - row)


def ring_shard(position, n):
    position = lax.rem(position + 2 * n, n)
    if n % 2:
        return position
    return jnp.where(position < n // 2, 2 * position, 2 * (n - 1 - position) + 1)


def kernel(
    experts,
    shards,
    limit,
    params,
    grads,
    moment,
    second,
    step,
    block_map,
    weights,
    new_moment,
    new_second,
    p_buf,
    g_buf,
    m_buf,
    s_buf,
    map_buf,
    tile,
    total_row,
    tiles,
    totals,
    load_sem,
    small_sem,
    tile_send,
    tile_recv,
    total_send,
    total_recv,
    ring_send,
    ring_recv,
):
    e = lax.axis_index("expert")
    s = lax.axis_index("shard")
    devices = experts * shards
    me = e * shards + s
    mats, rows, neurons = p_buf.shape
    width = rows * shards
    folds = neurons // LANES

    for k in range(mats):
        pltpu.make_async_copy(grads.at[k], g_buf.at[k], load_sem.at[0, k]).start()
    for k in range(mats):
        pltpu.make_async_copy(moment.at[k], m_buf.at[k], load_sem.at[1, k]).start()
        pltpu.make_async_copy(params.at[k], p_buf.at[k], load_sem.at[2, k]).start()

    map_load = pltpu.make_async_copy(block_map, map_buf, small_sem.at[0])
    second_load = pltpu.make_async_copy(second, s_buf, small_sem.at[1])
    map_load.start()
    second_load.start()

    barrier = pltpu.get_barrier_semaphore()

    def greet(j, carry):
        other = lax.rem(me + j, devices)
        pl.semaphore_signal(
            barrier,
            inc=1,
            device_id=(other // shards, lax.rem(other, shards)),
            device_id_type=MESH,
        )
        return carry

    lax.fori_loop(1, devices, greet, 0)

    blocks = second.shape[2]
    map_load.wait()
    second_load.wait()
    table = (
        lax.broadcasted_iota(jnp.int32, (blocks, neurons), 0) == map_buf[...]
    ).astype(jnp.float32)
    members = lax.dot_general(
        jnp.ones((8, neurons), jnp.float32),
        table,
        (((1,), (1,)), ((), ())),
        precision=lax.Precision.HIGHEST,
    )[:mats]
    step_value = jnp.full((1, LANES), step[0].astype(jnp.float32))
    first_fix = 1.0 - jnp.power(jnp.full((1, LANES), BETA_FIRST, jnp.float32), step_value)
    second_fix = 1.0 - jnp.power(jnp.full((1, LANES), BETA_SECOND, jnp.float32), step_value)
    first_fix = first_fix[:, :1]
    second_fix = second_fix[:, :1]

    squares = []
    for k in range(mats):
        pltpu.make_async_copy(grads.at[k], g_buf.at[k], load_sem.at[0, k]).wait()

        def add_squares(i, acc, k=k):
            g = g_buf[k, pl.ds(pl.multiple_of(i * STRIP, STRIP), STRIP), :]
            return acc + jnp.sum((g * g).reshape(STRIP // 8, 8, neurons), axis=0)

        acc = lax.fori_loop(0, rows // STRIP, add_squares, jnp.zeros((8, neurons), jnp.float32), unroll=2)
        squares.append(jnp.sum(acc, axis=0, keepdims=True))
    parts = [sq[:, f * LANES : (f + 1) * LANES] for f in range(folds) for sq in squares]
    own_total = functools.reduce(lambda a, b: a + b, parts)
    own_total = jnp.broadcast_to(jnp.sum(own_total, axis=1, keepdims=True), (1, LANES))
    pad = tile.shape[0] - len(parts)
    if pad:
        parts.append(jnp.zeros((pad, LANES), jnp.float32))
    own_tile = jnp.concatenate(parts, axis=0)
    tile[...] = own_tile
    total_row[...] = own_total
    tiles[s] = own_tile
    totals[me] = own_total

    pl.semaphore_wait(barrier, devices - 1)

    def tile_copy(j, arriving):
        to = lax.rem(s + j, shards)
        origin = lax.rem(s + shards - j, shards) if arriving else s
        return pltpu.make_async_remote_copy(
            src_ref=tile,
            dst_ref=tiles.at[origin],
            send_sem=tile_send.at[j],
            recv_sem=tile_recv.at[j],
            device_id=(e, to),
            device_id_type=MESH,
        )

    def total_copy(j, arriving):
        other = lax.rem(me + j, devices)
        origin = lax.rem(me + devices - j, devices) if arriving else me
        return pltpu.make_async_remote_copy(
            src_ref=total_row,
            dst_ref=totals.at[origin],
            send_sem=total_send.at[j],
            recv_sem=total_recv.at[j],
            device_id=(other // shards, lax.rem(other, shards)),
            device_id_type=MESH,
        )

    def start_total(j, carry):
        total_copy(j, False).start()
        return carry

    def start_tile(j, carry):
        tile_copy(j, False).start()
        return carry

    def wait_total(j, carry):
        total_copy(j, True).wait_recv()
        return carry

    def wait_tile(j, carry):
        tile_copy(j, True).wait_recv()
        return carry

    def sent_total(j, carry):
        total_copy(j, False).wait_send()
        return carry

    def sent_tile(j, carry):
        tile_copy(j, False).wait_send()
        return carry

    lax.fori_loop(1, devices, start_total, 0)
    lax.fori_loop(1, shards, start_tile, 0)
    lax.fori_loop(1, devices, wait_total, 0)
    lax.fori_loop(1, shards, wait_tile, 0)

    total = jnp.sum(totals[...], axis=0)
    clip = jnp.minimum(1.0, limit / (jnp.sqrt(total) + 1e-06))[:, :1]
    all_tile = jnp.sum(tiles[...], axis=0)
    square = jnp.concatenate(
        [all_tile[f * mats : (f + 1) * mats] for f in range(folds)], axis=1
    )
    block_sums = lax.dot_general(
        square, table, (((1,), (1,)), ((), ())), precision=lax.Precision.HIGHEST
    )
    updated = BETA_SECOND * s_buf[:, 0, :] + (1.0 - BETA_SECOND) * clip * clip * block_sums / (
        width * members
    )
    for k in range(mats):
        new_second[k] = updated[k : k + 1]
    divisor = jnp.sqrt(updated / second_fix) + epsilon
    by_neuron = lax.dot_general(
        divisor, table, (((1,), (0,)), ((), ())), precision=lax.Precision.HIGHEST
    )
    rate = LEARN_RATE / (first_fix * by_neuron)
    grad_scale = (1.0 - BETA_FIRST) * clip

    place = ring_position(s, shards)
    half = rows // 2
    right = ring_shard(place + 1, shards)
    left = ring_shard(place - 1, shards)
    far, near = shards // 2, (shards - 1) // 2
    hops = ((far, near), (near, far))

    def ring_copy(way, hop, k, part, arriving):
        back = hop + (1 if arriving else 0)
        origin = ring_shard(place - back if way == 0 else place + back, shards)
        block = weights.at[k, pl.ds(pl.multiple_of(origin * rows + part * half, half), half), :]
        return pltpu.make_async_remote_copy(
            src_ref=block,
            dst_ref=block,
            send_sem=ring_send.at[way, hop, 2 * k + part],
            recv_sem=ring_recv.at[way, hop, 2 * k + part],
            device_id=(e, right if way == 0 else left),
            device_id_type=MESH,
        )

    for k in range(mats):
        pltpu.make_async_copy(moment.at[k], m_buf.at[k], load_sem.at[1, k]).wait()
        pltpu.make_async_copy(params.at[k], p_buf.at[k], load_sem.at[2, k]).wait()
        rate_k = rate[k : k + 1]
        for part in range(2):

            def update(i, carry, k=k, part=part, rate_k=rate_k):
                at = pl.multiple_of(part * half + i * STRIP, STRIP)
                strip = pl.ds(at, STRIP)
                value = BETA_FIRST * m_buf[k, strip, :] + grad_scale * g_buf[k, strip, :]
                new_moment[k, strip, :] = value
                out = p_buf[k, strip, :] * (1.0 - LEARN_RATE * DECAY_WEIGHT) - rate_k * value
                weights[k, pl.ds(pl.multiple_of(s * rows + at, STRIP), STRIP), :] = out.astype(
                    jnp.bfloat16
                )
                return carry

            lax.fori_loop(0, half // STRIP, update, 0, unroll=2)
            for way in range(2):
                if hops[way][part] > 0:
                    ring_copy(way, 0, k, part, False).start()

    for hop in range(far):
        for k in range(mats):
            for part in range(2):
                for way in range(2):
                    if hop < hops[way][part]:
                        ring_copy(way, hop, k, part, True).wait_recv()
                        if hop + 1 < hops[way][part]:
                            ring_copy(way, hop + 1, k, part, False).start()
    for hop in range(far):
        for k in range(mats):
            for part in range(2):
                for way in range(2):
                    if hop < hops[way][part]:
                        ring_copy(way, hop, k, part, False).wait_send()
    lax.fori_loop(1, devices, sent_total, 0)
    lax.fori_loop(1, shards, sent_tile, 0)


def store_kernel(weights, moment, second, weights_out, moment_out, second_out, sem):
    mats = weights.shape[0]
    copies = [
        pltpu.make_async_copy(weights.at[k], weights_out.at[k], sem.at[0, k]) for k in range(mats)
    ] + [pltpu.make_async_copy(moment.at[k], moment_out.at[k], sem.at[1, k]) for k in range(mats)]
    copies.append(pltpu.make_async_copy(second, second_out, sem.at[0, mats]))
    for copy in copies:
        copy.start()
    for copy in copies:
        copy.wait()


def body(params, grads, moment, second, step, block_map):
    experts, shards = lax.axis_size("expert"), lax.axis_size("shard")
    mats, own, rows, neurons = params.shape
    blocks = second.shape[2]
    width = rows * shards
    devices = experts * shards
    limit = math.sqrt(mats * experts * own * width * neurons)
    flat = (mats, own * rows, neurons)
    far = max(shards // 2, 1)
    tile_rows = -(-mats * (neurons // LANES) // 8) * 8
    hbm = pl.BlockSpec(memory_space=pltpu.HBM)
    vmem = pl.BlockSpec(memory_space=pltpu.VMEM)
    smem = pl.BlockSpec(memory_space=pltpu.SMEM)
    dma = pltpu.SemaphoreType.DMA
    shapes = (
        jax.ShapeDtypeStruct((mats, width, neurons), jnp.bfloat16),
        jax.ShapeDtypeStruct(flat, jnp.float32),
        jax.ShapeDtypeStruct((mats, own, blocks), jnp.float32),
    )
    results = pl.pallas_call(
        functools.partial(kernel, experts, shards, limit),
        out_shape=tuple(pltpu.VMEM(shape.shape, shape.dtype) for shape in shapes),
        in_specs=[hbm, hbm, hbm, hbm, smem, hbm],
        out_specs=(vmem, vmem, vmem),
        scratch_shapes=[
            pltpu.VMEM(flat, jnp.float32),
            pltpu.VMEM(flat, jnp.float32),
            pltpu.VMEM(flat, jnp.float32),
            pltpu.VMEM((mats, own, blocks), jnp.float32),
            pltpu.VMEM((1, neurons), jnp.int32),
            pltpu.VMEM((tile_rows, LANES), jnp.float32),
            pltpu.VMEM((1, LANES), jnp.float32),
            pltpu.VMEM((shards, tile_rows, LANES), jnp.float32),
            pltpu.VMEM((devices, 1, LANES), jnp.float32),
            dma((3, mats)),
            dma((2,)),
            dma((shards,)),
            dma((shards,)),
            dma((devices,)),
            dma((devices,)),
            dma((2, far, 2 * mats)),
            dma((2, far, 2 * mats)),
        ],
        compiler_params=pltpu.CompilerParams(
            collective_id=0, has_side_effects=True, vmem_limit_bytes=46 * 1024 * 1024
        ),
    )(
        params.reshape(flat),
        grads.reshape(flat),
        moment.reshape(flat),
        second,
        step,
        block_map.reshape(1, neurons),
    )
    weights, new_moment, new_second = pl.pallas_call(
        store_kernel,
        out_shape=shapes,
        in_specs=[vmem, vmem, vmem],
        out_specs=(hbm, hbm, hbm),
        scratch_shapes=[dma((2, mats + 1))],
        compiler_params=pltpu.CompilerParams(vmem_limit_bytes=8 * 1024 * 1024),
    )(*results)
    return (
        weights.reshape(mats, own, width, neurons),
        new_moment.reshape(mats, own, rows, neurons),
        new_second,
    )


def solution(mesh):
    placed = (
        P(None, "expert", "shard", None),
        P(None, "expert", "shard", None),
        P(None, "expert", "shard", None),
        P(None, "expert", None),
        P(),
        P(),
    )
    return jax.shard_map(
        body,
        mesh=mesh,
        in_specs=placed,
        out_specs=(
            P(None, "expert", None, None),
            P(None, "expert", "shard", None),
            P(None, "expert", None),
        ),
        check_vma=False,
    )
```
